32 devices in a mesh: replica: 8 (over z, y), shard: 4 (over x, core).
Axes of the slice: x: 2, y: 2, z: 4, core: 2. Of those that a mesh axis runs over, the one named last changes fastest.
Arguments:
- outer_params: float32 [512, 4096], P('shard'), may hold values from -6 to 6, as said below
- local_params: bfloat16 [8, 512, 4096], P('replica', 'shard'), may hold values from -70 to 70
- momentum: float32 [512, 4096], P('shard'), may hold values from -6 to 6
Outputs:
- params_next: float32 [512, 4096], P('shard')
- momentum_next: float32 [512, 4096], P('shard')
- block_scales: float32 [32, 512], P(None, 'shard')
The draws below stay inside these ranges and needn't reach their ends.
Inputs may be any that keep to these rules, and one draw needn't show every extreme that they name: `outer_params`: outer parameters of order one.
All inputs are finite; a program needn't handle non-finite values.
Results may differ from the reference program's by a relative error of at most 0.005.
Values may be sent and summed in bfloat16 or wider, within the bound.
No kernel may reach another device: no remote copies, remote signals or barrier semaphores. Data moves between devices by JAX's collectives and lax.ppermute only.
A program may use at most 64 MiB of HBM per device.

```python
import math
import jax
import jax.numpy as jnp
from jax import lax

D = 4096
BLOCK = 128
ROWS = 512
WORKERS = 8


def draw_fields(key):
    base_key = jax.random.fold_in(key, 71)
    outer_key = jax.random.fold_in(base_key, 1)
    column_key = jax.random.fold_in(base_key, 2)
    common_key = jax.random.fold_in(base_key, 3)
    noise_key = jax.random.fold_in(base_key, 4)
    level_key = jax.random.fold_in(base_key, 5)
    group_rows = 32
    group_count = (ROWS + group_rows - 1) // group_rows
    raw_levels = jax.random.uniform(level_key, (group_count,), jnp.float32, 0.0, 1.0)
    unit_levels = raw_levels - jnp.max(raw_levels) + 1.0
    row_group = jnp.arange(ROWS, dtype=jnp.int32) // group_rows
    row_scale = 10.0 ** unit_levels[row_group]
    common_part = jnp.clip(jax.random.normal(common_key, (ROWS, D), jnp.float32), -4.0, 4.0)
    noise_part = jnp.clip(jax.random.normal(noise_key, (WORKERS, ROWS, D), jnp.float32), -4.0, 4.0)
    column_scale = jnp.exp(jax.random.uniform(column_key, (D,), jnp.float32, 0.0, math.log(10.0)))
    outer_values = jnp.clip(jax.random.normal(outer_key, (ROWS, D), jnp.float32), -6.0, 6.0)
    deltas = 0.05 * row_scale[:, None] * column_scale[None, :] * (common_part[None] + noise_part)
    return (outer_values, deltas)


def draw_outer_params(key, part):
    outer_values, deltas = draw_fields(key)
    return outer_values


def draw_local_params(key, part):
    outer_values, deltas = draw_fields(key)
    return (outer_values[None] - deltas).astype(jnp.bfloat16)


def block_scale(stream_key, extent, pieces, low, high):
    level = 1.0
    for axis_at, shards_of in pieces:
        draws = jax.random.uniform(jax.random.fold_in(jax.random.fold_in(stream_key, 6), axis_at), (shards_of,), jnp.float32, low / len(pieces), high / len(pieces))
        level = level * jnp.repeat(jnp.exp(draws), extent[axis_at] // shards_of).reshape((-1,) + (1,) * (len(extent) - 1 - axis_at))
    return level


def scatter_about(stream_key, dims, scale, most, pieces=(), kind=jnp.bfloat16):
    values = jax.random.normal(stream_key, dims, jnp.float32) * scale
    if len(pieces) > 0:
        values = block_scale(stream_key, dims, pieces, -0.22, 0.18) * values
    return jnp.clip(values, min=-most, max=most).astype(kind)


def setup_inputs(seed: int = 0) -> dict:
    seeds = jax.random.split(jax.random.key(seed), 4)
    outer_params = draw_outer_params(jax.random.fold_in(seeds[3], 71), 0)
    local_params = draw_local_params(jax.random.fold_in(seeds[3], 71), 0)
    momentum = scatter_about(seeds[2], (ROWS, D), 1.0, 6.0, ((0, 4),), jnp.float32)
    return {"outer_params": outer_params, "local_params": local_params, "momentum": momentum}


epsilon = 1e-06
clip_level = 0.5
outer_rate = 0.7
outer_decay = 0.9
grid_levels = 7.0

def smooth_step(values):
    return values - jnp.sin(2.0 * math.pi * values) / (2.0 * math.pi)

def smooth_round(values):
    return smooth_step(smooth_step(values))

def block_max(values):
    return lax.optimization_barrier(jnp.max(jnp.abs(values).reshape(values.shape[0], D // BLOCK, BLOCK), axis=2))

def reference(outer_params, local_params, momentum):

    def worker_max(running, worker_local):
        deltas = outer_params - worker_local.astype(jnp.float32)
        return (jnp.maximum(running, block_max(deltas)), None)
    absmax, _ = lax.scan(worker_max, jnp.zeros((ROWS, D // BLOCK), jnp.float32), local_params)
    spread_scale = jnp.repeat(absmax + epsilon, BLOCK, axis=1)

    def worker_sum(running, worker_local):
        deltas = outer_params - worker_local.astype(jnp.float32)
        encoded = smooth_round(grid_levels * deltas / spread_scale).astype(jnp.bfloat16)
        return (running + spread_scale * encoded.astype(jnp.float32) / grid_levels, None)
    summed_rows, _ = lax.scan(worker_sum, jnp.zeros((ROWS, D), jnp.float32), local_params)
    gradient = summed_rows / WORKERS
    root_mean = jnp.sqrt(jnp.mean(gradient * gradient) + epsilon)
    factor = jnp.minimum(1.0, clip_level / root_mean)
    clipped = factor * gradient
    momentum_next = outer_decay * momentum + clipped
    params_next = outer_params - outer_rate * (clipped + outer_decay * momentum_next)
    return (params_next, momentum_next, absmax.T)
```

```python
import functools
import math

import jax
import jax.numpy as jnp
from jax import lax
from jax.experimental import pallas as pl
from jax.experimental.pallas import tpu as pltpu
from jax.sharding import PartitionSpec as P


BLOCK = 128
LANES = 128

epsilon = 1e-06
clip_level = 0.5
outer_rate = 0.7
outer_decay = 0.9
grid_levels = 7.0

wire_scale = 512.0

step_poly = (
    6.57973575592041,
    -12.987854957580566,
    12.20757007598877,
    -6.687923908233643,
    2.3689229488372803,
    -0.5121645927429199,
)


def smooth_step_fraction(r):
    t = r * r
    f = step_poly[-1]
    for c in step_poly[-2::-1]:
        f = f * t + c
    return (r * t) * f


def smooth_round(values):
    whole = jnp.round(values)
    return whole + smooth_step_fraction(smooth_step_fraction(values - whole))


def absmax_kernel(q_ref, outer_ref, *refs):
    local_refs, out_ref = refs[:-1], refs[-1]
    rows, cols = outer_ref.shape
    lane = lax.broadcasted_iota(jnp.int32, (rows, LANES), 1)
    for first in range(0, cols // BLOCK, LANES):
        tile = jnp.zeros((rows, LANES), jnp.float32)
        for b in range(first, min(first + LANES, cols // BLOCK)):
            at = slice(b * BLOCK, (b + 1) * BLOCK)
            outer = outer_ref[:, at]
            most = None
            for ref in local_refs:
                local = ref[...] if ref.shape == (rows, cols) else ref[0]
                magnitude = jnp.abs(outer - ref[..., at].reshape(rows, BLOCK).astype(jnp.float32))
                most = magnitude if most is None else jnp.maximum(most, magnitude)
            block = jnp.max(most, axis=1, keepdims=True)
            tile = jnp.where(lane == b - first, block, tile)
        out_ref[:, first : first + LANES] = tile


def encode_kernel(per, first_block, q_ref, mine_ref, other_ref, outer_ref, *refs):
    local_refs, sum_ref, scale_ref = refs[:-2], refs[-2], refs[-1]
    rows, cols = outer_ref.shape
    absmax = jnp.maximum(mine_ref[...], other_ref[...])
    scale = absmax + epsilon
    inverse = grid_levels / scale
    weight = scale * per
    for b in range(cols // BLOCK):
        at = slice(b * BLOCK, (b + 1) * BLOCK)
        lane = slice(first_block + b, first_block + b + 1)
        outer = outer_ref[:, at]
        factor = jnp.broadcast_to(inverse[:, lane], (rows, BLOCK))
        total = None
        for ref in local_refs:
            delta = outer - ref[..., at].reshape(rows, BLOCK).astype(jnp.float32)
            code = smooth_round(delta * factor)
            total = code if total is None else total + code
        sum_ref[:, at] = total
        scale_ref[:, at] = jnp.broadcast_to(weight[:, lane], (rows, BLOCK))


def final_kernel(pieces, chunks, q_ref, factor_ref, outer_ref, momentum_ref, *refs):
    piece_refs, params_ref, next_ref = refs[:-2], refs[-2], refs[-1]
    cols = outer_ref.shape[1] // chunks
    factor = factor_ref[0] / wire_scale
    for k in range(pieces):

        @pl.when(pl.program_id(0) == k)
        def _():
            for c in range(chunks):
                at = slice(c * cols, (c + 1) * cols)
                clipped = factor * piece_refs[k * chunks + c][...]
                momentum_next = outer_decay * momentum_ref[:, at] + clipped
                next_ref[:, at] = momentum_next
                params_ref[:, at] = outer_ref[:, at] - outer_rate * (
                    clipped + outer_decay * momentum_next
                )


def tree_sum(values):
    while len(values) > 1:
        values = [values[i] + values[i + 1] for i in range(0, len(values), 2)]
    return values[0]


def per_device(outer_params, local_params, momentum):
    replicas = lax.axis_size("replica")
    shards = lax.axis_size("shard")
    row_count, col_count = outer_params.shape
    group = replicas // 2
    rows = row_count // group
    chunks = 2
    width = col_count // chunks
    blocks = col_count // BLOCK
    wide = -(-blocks // LANES) * LANES
    q = lax.axis_index("replica") % group
    q1 = q[None]
    vmem = pl.BlockSpec(memory_space=pltpu.VMEM)

    def swap(value, k):
        return lax.ppermute(
            value, "replica", [(i, (i // group) * group + (i % group ^ k)) for i in range(replicas)]
        )

    def cross(value):
        return lax.ppermute(value, "replica", [(i, (i + group) % replicas) for i in range(replicas)])

    def shard_swap(value, k):
        return lax.ppermute(value, "shard", [(i, i ^ k) for i in range(shards)])

    order = sorted(range(1, group), key=lambda k: -bin(k).count("1"))

    parts = local_params.reshape(group, rows, col_count)
    received = [swap(lax.dynamic_index_in_dim(parts, q ^ k, 0, keepdims=False), k) for k in order]

    row_spec = pl.BlockSpec((rows, col_count), lambda i, s: (s[0], 0))
    own_spec = pl.BlockSpec((1, rows, col_count), lambda i, s: (0, s[0], 0))
    whole_spec = pl.BlockSpec((rows, col_count), lambda i, s: (0, 0))
    absmax_half = pl.pallas_call(
        absmax_kernel,
        out_shape=jax.ShapeDtypeStruct((rows, wide), jnp.float32),
        grid_spec=pltpu.PrefetchScalarGridSpec(
            num_scalar_prefetch=1,
            grid=(1,),
            in_specs=[row_spec, own_spec] + [whole_spec] * len(received),
            out_specs=pl.BlockSpec((rows, wide), lambda i, s: (0, 0)),
        ),
        cost_estimate=pl.CostEstimate(flops=rows * col_count * group * 8, bytes_accessed=0, transcendentals=0),
        name="absmax",
    )(q1, outer_params, local_params, *received)
    absmax_other = cross(absmax_half)

    payloads = []
    squares = []
    for c in range(chunks):
        narrow = pl.BlockSpec((rows, wide), lambda i, s: (0, 0))
        half_sum, weight = pl.pallas_call(
            functools.partial(encode_kernel, 1.0 / (grid_levels * replicas), c * (width // BLOCK)),
            out_shape=[jax.ShapeDtypeStruct((rows, width), jnp.float32)] * 2,
            grid_spec=pltpu.PrefetchScalarGridSpec(
                num_scalar_prefetch=1,
                grid=(1,),
                in_specs=[
                    narrow,
                    narrow,
                    pl.BlockSpec((rows, width), lambda i, s, c=c: (s[0], c)),
                    pl.BlockSpec((1, rows, width), lambda i, s, c=c: (0, s[0], c)),
                ]
                + [pl.BlockSpec((rows, width), lambda i, s, c=c: (0, c))] * len(received),
                out_specs=[pl.BlockSpec((rows, width), lambda i, s: (0, 0))] * 2,
            ),
            cost_estimate=pl.CostEstimate(flops=rows * width * group * 40, bytes_accessed=0, transcendentals=0),
            name="encode",
        )(q1, absmax_half, absmax_other, outer_params, local_params, *received)
        mine = half_sum.astype(jnp.float16)
        other = cross(mine)
        gradient = (mine.astype(jnp.float32) + other.astype(jnp.float32)) * weight
        squares.append(jnp.sum(gradient * gradient))
        payloads.append((gradient * wire_scale).astype(jnp.float16))

    absmax = jnp.maximum(absmax_half, absmax_other)
    maxima = {k: swap(absmax, k) for k in order}
    maxima[0] = absmax
    pieces = [{k: swap(payload, k) for k in order} | {0: payload} for payload in payloads]

    total = sum(squares).reshape(1, 1)
    k = 1
    while k < shards:
        total = total + shard_swap(total, k)
        k *= 2
    sums = {k: swap(total, k) for k in order}
    sums[0] = total
    square_total = tree_sum([sums[k] for k in range(group)])
    entry_count = row_count * shards * col_count
    root_mean = jnp.sqrt(square_total / entry_count + epsilon)
    factor = jnp.minimum(1.0, clip_level / root_mean).reshape(1)

    by_row = pl.BlockSpec((rows, col_count), lambda i, s: (s[0] ^ i, 0))
    params_next, momentum_next = pl.pallas_call(
        functools.partial(final_kernel, group, chunks),
        out_shape=[jax.ShapeDtypeStruct((row_count, col_count), jnp.float32)] * 2,
        grid_spec=pltpu.PrefetchScalarGridSpec(
            num_scalar_prefetch=1,
            grid=(group,),
            in_specs=[pl.BlockSpec(memory_space=pltpu.SMEM), by_row, by_row] + [vmem] * (group * chunks),
            out_specs=[by_row, by_row],
        ),
        cost_estimate=pl.CostEstimate(flops=row_count * col_count * 8, bytes_accessed=0, transcendentals=0),
        name="outer_step",
    )(
        q1,
        factor,
        outer_params,
        momentum,
        *[pieces[c][k].astype(jnp.float32) for k in range(group) for c in range(chunks)],
    )
    stacked = jnp.concatenate([maxima[k][:, :blocks] for k in range(group)], axis=0).reshape(group, rows, blocks)
    ordered = jnp.take(stacked, jnp.arange(group) ^ q, axis=0).reshape(row_count, blocks)
    return (params_next, momentum_next, ordered.T)


def solution(mesh):
    return jax.shard_map(
        per_device,
        mesh=mesh,
        in_specs=(P("shard", None), P("replica", "shard", None), P("shard", None)),
        out_specs=(P("shard", None), P("shard", None), P(None, "shard")),
        check_vma=False,
    )
```
